32 devices in a mesh: rows: 8 (over y, x, core), cols: 4 (over z).
Axes of the slice: x: 2, y: 2, z: 4, core: 2. Of those that a mesh axis runs over, the one named last changes fastest.
Arguments:
- w_query: bfloat16 [4096, 4096], P('rows', 'cols'), may hold values from -0.09375 to 0.09375
- low_query: bfloat16 [4096, 16], P('rows'), may hold values from -0.09375 to 0.09375
- high_query: bfloat16 [16, 4096], P(None, 'cols'), may hold values from -1.5 to 1.5
- w_key: bfloat16 [4096, 1024], P('rows', 'cols'), may hold values from -0.09375 to 0.09375
- low_key: bfloat16 [4096, 16], P('rows'), may hold values from -0.09375 to 0.09375
- high_key: bfloat16 [16, 1024], P(None, 'cols'), may hold values from -1.5 to 1.5
- w_value: bfloat16 [4096, 1024], P('rows', 'cols'), may hold values from -0.09375 to 0.09375
- low_value: bfloat16 [4096, 16], P('rows'), may hold values from -0.09375 to 0.09375
- high_value: bfloat16 [16, 1024], P(None, 'cols'), may hold values from -1.5 to 1.5
- w_mixed: bfloat16 [4096, 4096], P('cols', 'rows'), may hold values from -0.09375 to 0.09375
- low_mixed: bfloat16 [4096, 16], P('cols'), may hold values from -0.09375 to 0.09375
- high_mixed: bfloat16 [16, 4096], P(None, 'rows'), may hold values from -1.5 to 1.5
- norm_train: float32 [4096], P(('rows', 'cols')), may hold values from 0.25 to 1.75
- norm_step: float32 [4096], P(('rows', 'cols')), may hold values from -0.3 to 0.3
Outputs:
- serving_query: bfloat16 [4096, 4096], P(None, 'cols')
- serving_key: bfloat16 [4096, 1024], P(None, 'cols')
- serving_value: bfloat16 [4096, 1024], P(None, 'cols')
- serving_mixed: bfloat16 [4096, 4096], P('cols')
- serve_norm: bfloat16 [4096], replicated
The draws below stay inside these ranges and needn't reach their ends.
All inputs are finite; a program needn't handle non-finite values.
Results may differ from the reference program's by a relative error of at most 0.001.
Values may be sent and summed in bfloat16 or wider, within the bound.
A program may use at most 128 MiB of HBM per device.

```python
import jax
import jax.numpy as jnp

D_MODEL = 4096
Q_DIM = 4096
KV_DIM = 1024
RANK = 16


def levels(own_key, dims, shards, low, largest):
    def one(axis_at, parts):
        draws = jax.random.uniform(jax.random.fold_in(jax.random.fold_in(own_key, 6), axis_at), (parts,), jnp.float32, low / len(shards), largest / len(shards))
        return jnp.repeat(jnp.exp(draws), dims[axis_at] // parts).reshape((-1,) + (1,) * (len(dims) - axis_at - 1))

    loudness = one(*shards[0])
    for cut in shards[1:]:
        loudness = loudness * one(*cut)
    return loudness


def noise(rng, extent, width, most, split=(), held_as=jnp.bfloat16):
    factor_of = levels(rng, extent, split, -0.22, 0.18) if split else 1.0
    values = jax.random.normal(rng, extent, jnp.float32) * width * factor_of
    return jnp.minimum(jnp.maximum(values, -most), most).astype(held_as)


def setup_inputs(seed: int = 0) -> dict:
    seeds = jax.random.split(jax.random.key(seed), 15)
    return {
        "w_query": noise(seeds[0], (D_MODEL, Q_DIM), D_MODEL ** -0.5, 0.09375, ((0, 8), (1, 4))),
        "low_query": noise(seeds[1], (D_MODEL, RANK), D_MODEL ** -0.5, 0.09375, ((0, 8),)),
        "high_query": noise(seeds[2], (RANK, Q_DIM), RANK ** -0.5, 1.5, ((1, 4),)),
        "w_key": noise(seeds[3], (D_MODEL, KV_DIM), D_MODEL ** -0.5, 0.09375, ((0, 8), (1, 4))),
        "low_key": noise(seeds[4], (D_MODEL, RANK), D_MODEL ** -0.5, 0.09375, ((0, 8),)),
        "high_key": noise(seeds[5], (RANK, KV_DIM), RANK ** -0.5, 1.5, ((1, 4),)),
        "w_value": noise(seeds[6], (D_MODEL, KV_DIM), D_MODEL ** -0.5, 0.09375, ((0, 8), (1, 4))),
        "low_value": noise(seeds[7], (D_MODEL, RANK), D_MODEL ** -0.5, 0.09375, ((0, 8),)),
        "high_value": noise(seeds[8], (RANK, KV_DIM), RANK ** -0.5, 1.5, ((1, 4),)),
        "w_mixed": noise(seeds[9], (Q_DIM, D_MODEL), Q_DIM ** -0.5, 0.09375, ((0, 4), (1, 8))),
        "low_mixed": noise(seeds[10], (Q_DIM, RANK), Q_DIM ** -0.5, 0.09375, ((0, 4),)),
        "high_mixed": noise(seeds[11], (RANK, D_MODEL), RANK ** -0.5, 1.5, ((1, 8),)),
        "norm_train": jnp.clip(1.0 + 0.15 * jax.random.normal(seeds[12], (D_MODEL,), jnp.float32), 0.25, 1.75),
        "norm_step": jnp.clip(jax.random.uniform(seeds[13], (D_MODEL,), jnp.float32, -0.3, 0.3) * levels(seeds[13], (D_MODEL,), ((0, 32),), -0.4, 0.0), -0.3, 0.3),
    }


mix_rate = 1.0


def reference(w_query, low_query, high_query, w_key, low_key, high_key, w_value, low_value, high_value, w_mixed, low_mixed, high_mixed, norm_train, norm_step):
    whole_query = w_query.astype(jnp.float32) + mix_rate * jnp.dot(low_query, high_query, preferred_element_type=jnp.float32)
    whole_key = w_key.astype(jnp.float32) + mix_rate * jnp.dot(low_key, high_key, preferred_element_type=jnp.float32)
    whole_value = w_value.astype(jnp.float32) + mix_rate * jnp.dot(low_value, high_value, preferred_element_type=jnp.float32)
    whole_mixed = w_mixed.astype(jnp.float32) + mix_rate * jnp.dot(low_mixed, high_mixed, preferred_element_type=jnp.float32)
    serving_query = whole_query.astype(jnp.bfloat16)
    serving_key = whole_key.astype(jnp.bfloat16)
    serving_value = whole_value.astype(jnp.bfloat16)
    serving_mixed = whole_mixed.astype(jnp.bfloat16)
    serve_norm = (norm_train + norm_step).astype(jnp.bfloat16)
    return serving_query, serving_key, serving_value, serving_mixed, serve_norm
```

```python
import functools

import jax
import jax.numpy as jnp
from jax import lax
from jax.experimental import pallas as pl
from jax.experimental.pallas import tpu as pltpu
from jax.sharding import PartitionSpec as P

mix_rate = 1.0
SIDE = 2
LINK_CHUNK = 1 << 17


def merged(weight, low, high):
    return (
        weight.astype(jnp.float32)
        + mix_rate * jnp.dot(low, high, preferred_element_type=jnp.float32)
    ).astype(jnp.bfloat16)


def plan_chunks(shapes):
    chunks = []
    for index, (height, width) in enumerate(shapes):
        rows = max(16, min(height // 2, LINK_CHUNK // (2 * width)))
        chunks += [(index, first, rows) for first in range(0, height, rows)]
    return chunks


def kernel(
    cols,
    chunks,
    split_dims,
    *refs,
):
    weights, lows, highs = refs[0:4], refs[4:8], refs[8:12]
    norm_train, norm_step = refs[12:14]
    outs, norm_out = refs[14:18], refs[18]
    held = refs[19:23]
    norm_slots, norm_rows = refs[23:25]
    load_sem, send_sem, x_sem, y_sem, far_sem, mate_sem, norm_send, norm_recv = refs[25:]

    me, col = lax.axis_index("rows"), lax.axis_index("cols")
    core, x, y = me % 2, (me // 2) % 2, me // 4

    def row_of(yy, xx, cc):
        return (yy * SIDE + xx) * 2 + cc

    side = row_of(y, 1 - x, core)
    across = row_of(1 - y, x, core)
    far = row_of(1 - y, 1 - x, core)
    mate = row_of(y, x, 1 - core)

    def place(owner, chunk):
        index, first, rows = chunk
        if split_dims[index] == 0:
            height = weights[index].shape[0]
            return outs[index].at[pl.ds(pl.multiple_of(owner * height + first, 16), rows), :]
        width = weights[index].shape[1]
        return outs[index].at[
            pl.ds(first, rows), pl.ds(pl.multiple_of(owner * width, 128), width)
        ]

    def shards(index, count):
        if split_dims[index] == 0:
            return outs[index].at[pl.ds(0, count * weights[index].shape[0]), :]
        return outs[index].at[:, pl.ds(0, count * weights[index].shape[1])]

    def send(owner, number, target, recv):
        chunk = chunks[number]
        where = place(owner, chunk)
        pltpu.make_async_remote_copy(
            src_ref=where,
            dst_ref=where,
            send_sem=send_sem.at[chunk[0]],
            recv_sem=recv,
            device_id=(target, col),
            device_id_type=pl.DeviceIdType.MESH,
        ).start()

    def arrived(owner, number, recv):
        where = place(owner, chunks[number])
        pltpu.make_async_copy(where, where, recv).wait()

    def load(number):
        index, first, rows = chunks[number]
        piece = pl.ds(first, rows)
        return pltpu.make_async_copy(
            weights[index].at[piece, :], held[index].at[piece, :], load_sem.at[number]
        )

    for number in range(len(chunks)):
        load(number).start()

    barrier = pltpu.get_barrier_semaphore()
    partners = [(lax.rem(me + step, 8), col) for step in range(1, 8)]
    mates = [(me, lax.rem(col + step, cols)) for step in range(1, cols)]
    for partner in partners + mates:
        pl.semaphore_signal(
            barrier, inc=1, device_id=partner, device_id_type=pl.DeviceIdType.MESH
        )
    norm_slots[me, col] = norm_train[...] + norm_step[...]
    pl.semaphore_wait(barrier, len(partners) + len(mates))

    def send_own(number):
        index = chunks[number][0]
        send(me, number, side, x_sem.at[number])
        send(me, number, across, y_sem.at[number])
        send(me, number, mate, mate_sem.at[index])

    for number, (index, first, rows) in enumerate(chunks):
        load(number).wait()
        piece = pl.ds(first, rows)
        place(me, chunks[number])[...] = merged(
            held[index][piece, :],
            lows[index][piece, :],
            highs[index][...],
        )
        if number:
            send_own(number - 1)

    def norm_copy(block, target, way):
        return pltpu.make_async_remote_copy(
            src_ref=block,
            dst_ref=block,
            send_sem=norm_send.at[way],
            recv_sem=norm_recv.at[way],
            device_id=target,
            device_id_type=pl.DeviceIdType.MESH,
        )

    for partner in mates:
        norm_copy(norm_slots.at[me, col], partner, 0).start()
    send_own(len(chunks) - 1)

    for number in range(len(chunks)):
        index = chunks[number][0]
        arrived(side, number, x_sem.at[number])
        if number % 2 == 0:
            send(side, number, across, far_sem.at[number])
        send(side, number, mate, mate_sem.at[index])
        arrived(across, number, y_sem.at[number])
        if number % 2 == 1:
            send(across, number, side, far_sem.at[number])
        send(across, number, mate, mate_sem.at[index])
        if number == 2:
            some = norm_slots.at[0, pl.ds(0, cols - 1)]
            pltpu.make_async_copy(some, some, norm_recv.at[0]).wait()
            pltpu.make_async_copy(some, some, norm_send.at[0]).wait()
            for partner in partners:
                norm_copy(norm_slots.at[me], partner, 1).start()

    some = norm_slots.at[pl.ds(0, 7)]
    pltpu.make_async_copy(some, some, norm_recv.at[1]).wait()
    pltpu.make_async_copy(some, some, norm_send.at[1]).wait()
    for row in range(8):
        for at in range(cols):
            norm_rows[pl.ds(row * cols + at, 1), :] = norm_slots[row, at]
    norm_out[...] = norm_rows[...].astype(jnp.bfloat16)

    for number in range(len(chunks)):
        arrived(far, number, far_sem.at[number])
        send(far, number, mate, mate_sem.at[chunks[number][0]])

    for index in range(4):
        some = shards(index, 4)
        pltpu.make_async_copy(some, some, mate_sem.at[index]).wait()
        some = shards(index, 7)
        pltpu.make_async_copy(some, some, send_sem.at[index]).wait()


def gather_kernel(cols, weights, lows, highs, norm_train, norm_step):
    split_dims = (0, 0, 0, 1)
    shapes = [weight.shape for weight in weights]
    chunks = plan_chunks(shapes)
    full = [
        (height * 8, width) if dim == 0 else (height, width * 8)
        for (height, width), dim in zip(shapes, split_dims)
    ]
    rows, width = 8 * cols, norm_train.shape[0]
    whole = pl.BlockSpec(memory_space=pltpu.VMEM)
    count = len(chunks)
    results = pl.pallas_call(
        functools.partial(kernel, cols, chunks, split_dims),
        out_shape=[pltpu.VMEM(shape, jnp.bfloat16) for shape in full]
        + [jax.ShapeDtypeStruct((rows, width), jnp.bfloat16)],
        in_specs=[pl.BlockSpec(memory_space=pl.ANY)] * 4 + [whole] * 10,
        out_specs=[pl.BlockSpec(memory_space=pltpu.VMEM)] * 5,
        scratch_shapes=[pltpu.VMEM(shape, jnp.bfloat16) for shape in shapes]
        + [
            pltpu.VMEM((8, cols, 1, width), jnp.float32),
            pltpu.VMEM((rows, width), jnp.float32),
            pltpu.SemaphoreType.DMA((count,)),
            pltpu.SemaphoreType.DMA((4,)),
            pltpu.SemaphoreType.DMA((count,)),
            pltpu.SemaphoreType.DMA((count,)),
            pltpu.SemaphoreType.DMA((count,)),
            pltpu.SemaphoreType.DMA((4,)),
            pltpu.SemaphoreType.DMA((2,)),
            pltpu.SemaphoreType.DMA((2,)),
        ],
        compiler_params=pltpu.CompilerParams(
            collective_id=0, has_side_effects=True, vmem_limit_bytes=VMEM_LIMIT
        ),
    )(*weights, *lows, *highs, norm_train.reshape(1, width), norm_step.reshape(1, width))
    return (*results[:4], results[4].reshape(rows * width))


VMEM_LIMIT = 30 << 20


def local(
    rows,
    cols,
    w_query,
    low_query,
    high_query,
    w_key,
    low_key,
    high_key,
    w_value,
    low_value,
    high_value,
    w_mixed,
    low_mixed,
    high_mixed,
    norm_train,
    norm_step,
):
    weights = (w_query, w_key, w_value, w_mixed)
    lows = (low_query, low_key, low_value, low_mixed)
    highs = (high_query, high_key, high_value, high_mixed)
    if rows == SIDE * SIDE * 2 and cols > 1:
        return gather_kernel(cols, weights, lows, highs, norm_train, norm_step)
    pieces = [merged(*parts) for parts in zip(weights, lows, highs)]
    gathered = [
        lax.all_gather(piece, "rows", axis=axis, tiled=True)
        for piece, axis in zip(pieces, (0, 0, 0, 1))
    ]
    norm = lax.all_gather(
        (norm_train + norm_step).astype(jnp.bfloat16), ("rows", "cols"), axis=0, tiled=True
    )
    return (*gathered, norm)


def solution(mesh):
    in_specs = (
        P("rows", "cols"),
        P("rows", None),
        P(None, "cols"),
        P("rows", "cols"),
        P("rows", None),
        P(None, "cols"),
        P("rows", "cols"),
        P("rows", None),
        P(None, "cols"),
        P("cols", "rows"),
        P("cols", None),
        P(None, "rows"),
        P(("rows", "cols")),
        P(("rows", "cols")),
    )
    out_specs = (P(None, "cols"), P(None, "cols"), P(None, "cols"), P("cols", None), P())
    body = functools.partial(local, mesh.shape["rows"], mesh.shape["cols"])
    return jax.shard_map(body, mesh=mesh, in_specs=in_specs, out_specs=out_specs, check_vma=False)
```

```python
import functools

import jax
import jax.numpy as jnp
from jax import lax
from jax.experimental import pallas as pl
from jax.experimental.pallas import tpu as pltpu
from jax.sharding import PartitionSpec as P

mix_rate = 1.0
SIDE = 2
LINK_CHUNK = 1 << 17


def merged(weight, low, high):
    return (
        weight.astype(jnp.float32)
        + mix_rate * jnp.dot(low, high, preferred_element_type=jnp.float32)
    ).astype(jnp.bfloat16)


def plan_chunks(shapes):
    chunks = []
    for index, (height, width) in enumerate(shapes):
        rows = max(16, min(height // 2, LINK_CHUNK // (2 * width)))
        chunks += [(index, first, rows) for first in range(0, height, rows)]
    return chunks


def kernel(
    cols,
    chunks,
    split_dims,
    *refs,
):
    weights, lows, highs = refs[0:4], refs[4:8], refs[8:12]
    norms = refs[12:14]
    outs, norm_out = refs[14:18], refs[18]
    held, held_lows, held_highs, turned = refs[19:23], refs[23:27], refs[27:31], refs[31:35]
    held_norms, norm_slots, norm_rows = refs[35:37], refs[37], refs[38]
    load_sem, small_sem, send_sem, x_sem, y_sem, far_sem, mate_sem, norm_send, norm_recv = refs[39:]

    me, col = lax.axis_index("rows"), lax.axis_index("cols")
    core, x, y = me % 2, (me // 2) % 2, me // 4

    def row_of(yy, xx, cc):
        return (yy * SIDE + xx) * 2 + cc

    side = row_of(y, 1 - x, core)
    across = row_of(1 - y, x, core)
    far = row_of(1 - y, 1 - x, core)
    mate = row_of(y, x, 1 - core)

    def place(owner, chunk):
        index, first, rows = chunk
        if split_dims[index] == 0:
            height = weights[index].shape[0]
            return outs[index].at[pl.ds(pl.multiple_of(owner * height + first, 16), rows), :]
        width = weights[index].shape[1]
        return outs[index].at[
            pl.ds(first, rows), pl.ds(pl.multiple_of(owner * width, 128), width)
        ]

    def shards(index, count):
        if split_dims[index] == 0:
            return outs[index].at[pl.ds(0, count * weights[index].shape[0]), :]
        return outs[index].at[:, pl.ds(0, count * weights[index].shape[1])]

    def send(owner, number, target, recv):
        chunk = chunks[number]
        where = place(owner, chunk)
        pltpu.make_async_remote_copy(
            src_ref=where,
            dst_ref=where,
            send_sem=send_sem.at[chunk[0]],
            recv_sem=recv,
            device_id=(target, col),
            device_id_type=pl.DeviceIdType.MESH,
        ).start()

    def arrived(owner, number, recv):
        where = place(owner, chunks[number])
        pltpu.make_async_copy(where, where, recv).wait()

    def load(number):
        index, first, rows = chunks[number]
        piece = pl.ds(first, rows)
        return pltpu.make_async_copy(
            weights[index].at[piece, :], held[index].at[piece, :], load_sem.at[number]
        )

    def small_load(number):
        source = (*lows, *highs, *norms)[number]
        target = (*held_lows, *held_highs, *held_norms)[number]
        return pltpu.make_async_copy(source, target, small_sem.at[number])

    barrier = pltpu.get_barrier_semaphore()
    partners = [(lax.rem(me + step, 8), col) for step in range(1, 8)]
    mates = [(me, lax.rem(col + step, cols)) for step in range(1, cols)]
    for partner in partners + mates:
        pl.semaphore_signal(
            barrier, inc=1, device_id=partner, device_id_type=pl.DeviceIdType.MESH
        )
    begun = set()
    for number in range(len(chunks)):
        index = chunks[number][0]
        if index not in begun:
            begun.add(index)
            small_load(index).start()
            small_load(4 + index).start()
        load(number).start()
    small_load(8).start()
    small_load(9).start()
    pl.semaphore_wait(barrier, len(partners) + len(mates))

    def send_own(number):
        index = chunks[number][0]
        send(me, number, side, x_sem.at[number])
        send(me, number, across, y_sem.at[number])
        send(me, number, mate, mate_sem.at[index])

    ready = set()
    for number, (index, first, rows) in enumerate(chunks):
        if index not in ready:
            ready.add(index)
            small_load(index).wait()
            small_load(4 + index).wait()
            turned[index][...] = held_lows[index][...].astype(jnp.float32).T.astype(jnp.bfloat16)
        load(number).wait()
        piece = pl.ds(first, rows)
        place(me, chunks[number])[...] = merged(
            held[index][piece, :],
            turned[index][piece, :],
            held_highs[index][...],
        )
        if number:
            send_own(number - 1)

    def norm_copy(block, target, way):
        return pltpu.make_async_remote_copy(
            src_ref=block,
            dst_ref=block,
            send_sem=norm_send.at[way],
            recv_sem=norm_recv.at[way],
            device_id=target,
            device_id_type=pl.DeviceIdType.MESH,
        )

    small_load(8).wait()
    small_load(9).wait()
    norm_slots[me, col] = held_norms[0][...] + held_norms[1][...]
    for partner in mates:
        norm_copy(norm_slots.at[me, col], partner, 0).start()
    send_own(len(chunks) - 1)

    for number in range(len(chunks)):
        index = chunks[number][0]
        arrived(side, number, x_sem.at[number])
        if number % 2 == 0:
            send(side, number, across, far_sem.at[number])
        send(side, number, mate, mate_sem.at[index])
        arrived(across, number, y_sem.at[number])
        if number % 2 == 1:
            send(across, number, side, far_sem.at[number])
        send(across, number, mate, mate_sem.at[index])
        if number == 2:
            some = norm_slots.at[0, pl.ds(0, cols - 1)]
            pltpu.make_async_copy(some, some, norm_recv.at[0]).wait()
            pltpu.make_async_copy(some, some, norm_send.at[0]).wait()
            for partner in partners:
                norm_copy(norm_slots.at[me], partner, 1).start()

    some = norm_slots.at[pl.ds(0, 7)]
    pltpu.make_async_copy(some, some, norm_recv.at[1]).wait()
    pltpu.make_async_copy(some, some, norm_send.at[1]).wait()
    for row in range(8):
        for at in range(cols):
            norm_rows[pl.ds(row * cols + at, 1), :] = norm_slots[row, at]
    norm_out[...] = norm_rows[...].astype(jnp.bfloat16)

    for number in range(len(chunks)):
        arrived(far, number, far_sem.at[number])
        send(far, number, mate, mate_sem.at[chunks[number][0]])

    for index in range(4):
        some = shards(index, 4)
        pltpu.make_async_copy(some, some, mate_sem.at[index]).wait()
        some = shards(index, 7)
        pltpu.make_async_copy(some, some, send_sem.at[index]).wait()


def gather_kernel(cols, weights, lows, highs, norm_train, norm_step):
    split_dims = (0, 0, 0, 1)
    lows = [low.T for low in lows]
    shapes = [weight.shape for weight in weights]
    chunks = plan_chunks(shapes)
    full = [
        (height * 8, width) if dim == 0 else (height, width * 8)
        for (height, width), dim in zip(shapes, split_dims)
    ]
    rows, width = 8 * cols, norm_train.shape[0]
    whole = pl.BlockSpec(memory_space=pltpu.VMEM)
    count = len(chunks)
    kept = 2 * (sum(height * across for height, across in full) + rows * width)
    results = pl.pallas_call(
        functools.partial(kernel, cols, chunks, split_dims),
        out_shape=[pltpu.VMEM(shape, jnp.bfloat16) for shape in full]
        + [pltpu.VMEM((rows, width), jnp.bfloat16)],
        in_specs=[pl.BlockSpec(memory_space=pltpu.HBM)] * 14,
        out_specs=[whole] * 5,
        scratch_shapes=[pltpu.VMEM(shape, jnp.bfloat16) for shape in shapes]
        + [pltpu.VMEM(low.shape, jnp.bfloat16) for low in lows]
        + [pltpu.VMEM(high.shape, jnp.bfloat16) for high in highs]
        + [pltpu.VMEM(low.shape[::-1], jnp.bfloat16) for low in lows]
        + [pltpu.VMEM((1, width), jnp.float32)] * 2
        + [
            pltpu.VMEM((8, cols, 1, width), jnp.float32),
            pltpu.VMEM((rows, width), jnp.float32),
            pltpu.SemaphoreType.DMA((count,)),
            pltpu.SemaphoreType.DMA((10,)),
            pltpu.SemaphoreType.DMA((4,)),
            pltpu.SemaphoreType.DMA((count,)),
            pltpu.SemaphoreType.DMA((count,)),
            pltpu.SemaphoreType.DMA((count,)),
            pltpu.SemaphoreType.DMA((4,)),
            pltpu.SemaphoreType.DMA((2,)),
            pltpu.SemaphoreType.DMA((2,)),
        ],
        compiler_params=pltpu.CompilerParams(
            collective_id=0, has_side_effects=True, vmem_limit_bytes=VMEM_BYTES - kept
        ),
    )(*weights, *lows, *highs, norm_train.reshape(1, width), norm_step.reshape(1, width))
    results = write_out(results)
    return (*results[:4], results[4].reshape(rows * width))


VMEM_BYTES = 67043328
WRITE_PIECES = 4


def write_kernel(*refs):
    count = len(refs) // 2
    sources, targets, sem = refs[:count], refs[count:-1], refs[-1]
    copies = []
    for index in range(count):
        height = sources[index].shape[0]
        pieces = WRITE_PIECES if height >= 1024 else 1
        for piece in range(pieces):
            part = pl.ds(piece * (height // pieces), height // pieces)
            copies.append(
                pltpu.make_async_copy(
                    sources[index].at[part, :],
                    targets[index].at[part, :],
                    sem.at[index * WRITE_PIECES + piece],
                )
            )
            copies[-1].start()
    for copy in copies:
        copy.wait()


def write_out(arrays):
    return pl.pallas_call(
        write_kernel,
        out_shape=[jax.ShapeDtypeStruct(array.shape, array.dtype) for array in arrays],
        in_specs=[pl.BlockSpec(memory_space=pltpu.VMEM)] * len(arrays),
        out_specs=[pl.BlockSpec(memory_space=pltpu.HBM)] * len(arrays),
        scratch_shapes=[pltpu.SemaphoreType.DMA((len(arrays) * WRITE_PIECES,))],
        compiler_params=pltpu.CompilerParams(vmem_limit_bytes=WRITE_LIMIT),
    )(*arrays)


WRITE_LIMIT = 1 << 20


def local(
    rows,
    cols,
    w_query,
    low_query,
    high_query,
    w_key,
    low_key,
    high_key,
    w_value,
    low_value,
    high_value,
    w_mixed,
    low_mixed,
    high_mixed,
    norm_train,
    norm_step,
):
    weights = (w_query, w_key, w_value, w_mixed)
    lows = (low_query, low_key, low_value, low_mixed)
    highs = (high_query, high_key, high_value, high_mixed)
    if rows == SIDE * SIDE * 2 and cols > 1:
        return gather_kernel(cols, weights, lows, highs, norm_train, norm_step)
    pieces = [merged(*parts) for parts in zip(weights, lows, highs)]
    gathered = [
        lax.all_gather(piece, "rows", axis=axis, tiled=True)
        for piece, axis in zip(pieces, (0, 0, 0, 1))
    ]
    norm = lax.all_gather(
        (norm_train + norm_step).astype(jnp.bfloat16), ("rows", "cols"), axis=0, tiled=True
    )
    return (*gathered, norm)


def solution(mesh):
    in_specs = (
        P("rows", "cols"),
        P("rows", None),
        P(None, "cols"),
        P("rows", "cols"),
        P("rows", None),
        P(None, "cols"),
        P("rows", "cols"),
        P("rows", None),
        P(None, "cols"),
        P("cols", "rows"),
        P("cols", None),
        P(None, "rows"),
        P(("rows", "cols")),
        P(("rows", "cols")),
    )
    out_specs = (P(None, "cols"), P(None, "cols"), P(None, "cols"), P("cols", None), P())
    body = functools.partial(local, mesh.shape["rows"], mesh.shape["cols"])
    return jax.shard_map(body, mesh=mesh, in_specs=in_specs, out_specs=out_specs, check_vma=False)
```
